32 devices in a mesh: groups: 2 (over x), blk: 8 (over z, y), rep: 2 (over core).
Axes of the slice: x: 2, y: 2, z: 4, core: 2. Of those that a mesh axis runs over, the one named last changes fastest.
Arguments:
- tokens: bfloat16 [2048, 7168], P(('groups', 'blk', 'rep')), parts along dimension 0, may hold values from -6 to 6
- router_scores: float32 [2048, 8], P(('groups', 'blk', 'rep')), parts along dimension 0, may hold values from -6 to 6
- expert_ids: int32 [2048, 8], P(('groups', 'blk', 'rep')), parts along dimension 0, may hold values from 0 to 255, as said below
- gate_weight: bfloat16 [7168, 4096], P(None, ('blk', 'rep')), may hold values from -0.0625 to 0.0625
- up_weight: bfloat16 [7168, 4096], P(None, ('blk', 'rep')), may hold values from -0.0625 to 0.0625
- down_weight: bfloat16 [4096, 7168], P(('blk', 'rep')), may hold values from -0.125 to 0.125
Outputs:
- moe_out: bfloat16 [2048, 7168], P(('groups', 'blk', 'rep')), parts along dimension 0
The draws below stay inside these ranges and needn't reach their ends.
There are 2 independent parts, one for each index of `groups`. The reference program is written for one: setup_inputs(seed, part) draws one part's arguments, and reference() takes and returns one part's arrays. A program takes and returns all parts, laid end to end along the dimension named above; an argument that names none is the same for every part. Nothing has to cross between parts.
Inputs may be any that keep to these rules, and one draw needn't show every extreme that they name: `expert_ids`: each row names 8 different experts. In the rows of one device (aligned blocks of 64 rows) each expert below 2 is named by at most 2 rows, and in every draw one such expert is named by exactly 2 rows in every block.
All inputs are finite; a program needn't handle non-finite values.
Results may differ from the reference program's by a relative error of at most 0.0068.
Values may be sent and summed in bfloat16 or wider, within the bound.
A program may use at most 128 MiB of HBM per device.

```python
import jax
import jax.numpy as jnp
from jax import lax

D = 7168
FF = 2048
EXPERTS = 256
TOP = 8
TOK_DEV = 64
CAP = 2
EXP_WIN = 2
TOKENS = 1024


def draw_block(block_key, hot_expert, expert_caps):
    key_count, key_rows, key_offset, key_order = jax.random.split(block_key, 4)
    counts = jax.random.randint(key_count, (EXP_WIN,), 0, expert_caps + 1)
    counts = jnp.where(jnp.arange(EXP_WIN) == hot_expert, CAP, counts)
    item_ends = jnp.cumsum(counts)
    total_items = item_ends[-1]
    item_index = jnp.arange(EXP_WIN * CAP)
    owners = jnp.sum((item_ends[None, :] <= item_index[:, None]).astype(jnp.int32), axis=1)
    is_valid = item_index < total_items
    row_order = jax.random.permutation(key_rows, TOK_DEV)
    item_row = jnp.where(is_valid, row_order[item_index % TOK_DEV], TOK_DEV)
    item_slot = item_index // TOK_DEV
    offsets = jax.random.randint(key_offset, (TOK_DEV, 1), 0, EXPERTS - EXP_WIN)
    outer_ids = EXP_WIN + (offsets + jnp.arange(TOP)[None, :]) % (EXPERTS - EXP_WIN)
    id_table = outer_ids.at[item_row, item_slot].set(owners, mode='drop')
    order_keys = jax.random.split(key_order, TOK_DEV)
    orders = jax.vmap(lambda one_key: jax.random.permutation(one_key, TOP))(order_keys)
    return jnp.take_along_axis(id_table, orders, axis=1).astype(jnp.int32)


def draw_expert_ids(key, part):
    num_blocks = TOKENS // TOK_DEV
    key_hot, key_caps, key_rest = jax.random.split(key, 3)
    hot_expert = jax.random.randint(key_hot, (), 0, EXP_WIN)
    expert_caps = jax.random.randint(key_caps, (EXP_WIN,), CAP // 2, CAP + 1)
    block_keys = jax.random.split(key_rest, num_blocks)
    id_blocks = jax.vmap(lambda one_key: draw_block(one_key, hot_expert, expert_caps))(block_keys)
    return id_blocks.reshape(TOKENS, TOP).astype(jnp.int32)


def steps_of(own_key, shape, cuts, low, high):
    def one(axis_at, shards_of):
        heights = jax.random.uniform(jax.random.fold_in(jax.random.fold_in(own_key, 6), axis_at), (shards_of,), jnp.float32, low / len(cuts), high / len(cuts))
        return jnp.repeat(jnp.exp(heights), shape[axis_at] // shards_of).reshape((-1,) + (1,) * (len(shape) - axis_at - 1))

    loudness = one(*cuts[0])
    for cut in cuts[1:]:
        loudness = loudness * one(*cut)
    return loudness


def noise(rng, dims, spread, most, pieces=(), kind=jnp.bfloat16):
    values = spread * jax.random.normal(rng, dims, jnp.float32)
    if pieces:
        values = values * steps_of(rng, dims, pieces, -0.22, 0.18)
    return jnp.clip(values, -most, most).astype(kind)


def setup_inputs(seed: int = 0, part: int = 0) -> dict:
    key_of = jax.random.split(jax.random.key(seed), 7)
    part_splits = jax.random.split(jax.random.fold_in(key_of[6], part), 7)
    return {
        "tokens": noise(part_splits[0], (TOKENS, D), 1.0, 6.0, ((0, 16),)),
        "router_scores": noise(part_splits[1], (TOKENS, TOP), 1.5, 6.0, ((0, 16),), jnp.float32),
        "expert_ids": draw_expert_ids(jax.random.fold_in(jax.random.fold_in(key_of[6], part), 71), part),
        "gate_weight": noise(key_of[3], (D, EXP_WIN * FF), D ** -0.5, 0.0625, ((1, 16),)),
        "up_weight": noise(key_of[4], (D, EXP_WIN * FF), D ** -0.5, 0.0625, ((1, 16),)),
        "down_weight": noise(key_of[5], (EXP_WIN * FF, D), FF ** -0.5, 0.125, ((0, 16),)),
    }


route_scale = 2.5


def reference(tokens, router_scores, expert_ids, gate_weight, up_weight, down_weight):
    sigmoid_scores = jax.nn.sigmoid(router_scores.astype(jnp.float32))
    gate_values = route_scale * sigmoid_scores / jnp.sum(sigmoid_scores, axis=1, keepdims=True)
    row_limit = CAP * (TOKENS // TOK_DEV)

    def one_expert(running, expert):
        member = expert_ids == expert
        weight_row = jnp.sum(jnp.where(member, gate_values, jnp.float32(0.0)), axis=1)
        is_named = jnp.any(member, axis=1)
        named_count = jnp.sum(is_named.astype(jnp.int32))
        positions = jnp.nonzero(is_named, size=row_limit, fill_value=0)[0].astype(jnp.int32)
        is_valid = jnp.arange(row_limit, dtype=jnp.int32) < named_count
        picked_rows = tokens[positions]
        first_unit = (expert * FF).astype(jnp.int32)
        w_gate = lax.dynamic_slice_in_dim(gate_weight, first_unit, FF, 1)
        w_up = lax.dynamic_slice_in_dim(up_weight, first_unit, FF, 1)
        w_down = lax.dynamic_slice_in_dim(down_weight, first_unit, FF, 0)
        gate_proj = jnp.dot(picked_rows, w_gate, preferred_element_type=jnp.float32)
        up_proj = jnp.dot(picked_rows, w_up, preferred_element_type=jnp.float32)
        hidden = (jax.nn.silu(gate_proj) * up_proj).astype(jnp.bfloat16)
        expert_out = jnp.dot(hidden, w_down, preferred_element_type=jnp.float32)
        row_weight = jnp.where(is_valid, weight_row[positions], jnp.float32(0.0))
        running = running.at[positions].add(row_weight[:, None] * expert_out)
        return running, None

    start_value = jnp.zeros((TOKENS, D), jnp.float32)
    combined, _ = lax.scan(one_expert, start_value, jnp.arange(EXP_WIN, dtype=jnp.int32))
    return combined.astype(jnp.bfloat16)
```

```python
import functools

import jax
import jax.numpy as jnp
from jax import lax
from jax.experimental import pallas as pl
from jax.experimental.pallas import tpu as pltpu
from jax.sharding import PartitionSpec as P

FF = 2048
CAP = 2
MESH = pl.DeviceIdType.MESH

route_scale = 2.5


def kernel(
    blks, reps, experts, kchunks, nchunks,
    scores_ref, ids_ref, tok_hbm, gate_hbm, up_hbm, down_hbm, out_ref,
    tok, wg, wu, wd, packed, rows, keep, give, got, back, returned, weight_buf,
    tok_sem, w_sem, d_sem, dsend, recv, fsend, ysend, xsend, xrecv, bsend, brecv,
):
    b = lax.axis_index("blk")
    r = lax.axis_index("rep")
    sib = 1 - r
    group = blks // experts
    half = group // 2
    width = tok.shape[1]
    slots = experts * CAP
    kc = width // kchunks
    nc = width // nchunks
    parity = lax.rem(b, 2)
    own_q = lax.div(b, 2)
    own_expert = lax.div(b, group)
    quads = blks // 2

    tok_copy = pltpu.make_async_copy(tok_hbm, tok, tok_sem)
    tok_copy.start()

    def k_copies(k):
        at = pl.ds(k * kc, kc)
        return (
            pltpu.make_async_copy(gate_hbm.at[at, :], wg.at[at, :], w_sem.at[0, k]),
            pltpu.make_async_copy(up_hbm.at[at, :], wu.at[at, :], w_sem.at[1, k]),
        )

    def d_copy(n):
        at = pl.ds(n * nc, nc)
        return pltpu.make_async_copy(down_hbm.at[:, at], wd.at[:, at], d_sem.at[n])

    for k in range(kchunks):
        for copy in k_copies(k):
            copy.start()
    for n in range(nchunks):
        d_copy(n).start()

    barrier = pltpu.get_barrier_semaphore()
    for rr in range(reps):
        @pl.loop(0, blks)
        def _(bb):
            @pl.when(jnp.logical_or(bb != b, rr != r))
            def _():
                pl.semaphore_signal(
                    barrier, inc=1, device_id={"blk": bb, "rep": rr}, device_id_type=MESH
                )

    sig = jax.nn.sigmoid(scores_ref[...])
    gates = route_scale * sig / jnp.sum(sig, axis=1, keepdims=True)
    ids = ids_ref[...]
    t_count = ids.shape[0]
    slot = lax.broadcasted_iota(jnp.int32, (t_count, slots), 1)
    slot_expert = lax.div(slot, CAP)
    slot_rank = (slot - slot_expert * CAP).astype(jnp.float32)
    hit = jnp.zeros((t_count, slots), jnp.float32)
    weight = jnp.zeros((t_count, slots), jnp.float32)
    for j in range(ids.shape[1]):
        same = ids[:, j : j + 1] == slot_expert
        hit = hit + jnp.where(same, 1.0, 0.0)
        weight = weight + jnp.where(same, gates[:, j : j + 1], 0.0)
    row_i = lax.broadcasted_iota(jnp.int32, (t_count, t_count), 0)
    col_i = lax.broadcasted_iota(jnp.int32, (t_count, t_count), 1)
    lower = jnp.where(col_i <= row_i, 1.0, 0.0).astype(jnp.bfloat16)
    rank = jnp.dot(lower, hit.astype(jnp.bfloat16), preferred_element_type=jnp.float32) - 1.0
    placed = jnp.where(rank == slot_rank, hit, 0.0)
    weight_buf[...] = placed * weight
    tok_copy.wait()
    picked = lax.dot_general(
        placed.astype(jnp.bfloat16), tok[...], (((0,), (0,)), ((), ())),
        preferred_element_type=jnp.float32,
    ).astype(jnp.bfloat16)
    for e in range(experts):
        packed[e] = picked[e * CAP : (e + 1) * CAP, :]

    pl.semaphore_wait(barrier, blks * reps - 1)

    def first(e, h):
        dst = e * group + 2 * h + parity
        copy = pltpu.make_async_remote_copy(
            src_ref=packed.at[e], dst_ref=rows.at[r, b],
            send_sem=dsend.at[e * half + h], recv_sem=recv.at[r, b],
            device_id={"blk": dst, "rep": r}, device_id_type=MESH,
        )
        return dst, copy

    own_copy = pltpu.make_async_copy(packed.at[own_expert], rows.at[r, b], recv.at[r, b])
    own_copy.start()

    @pl.loop(0, experts)
    def _(e):
        @pl.loop(0, half)
        def _(h):
            dst, copy = first(e, h)

            @pl.when(dst != b)
            def _():
                copy.start()

    def landed(rr, bb):
        return pltpu.make_async_copy(rows.at[rr, bb], rows.at[rr, bb], recv.at[rr, bb])

    def forward(bb, sems, dst_b, dst_r):
        return pltpu.make_async_remote_copy(
            src_ref=rows.at[r, bb], dst_ref=rows.at[r, bb],
            send_sem=sems.at[bb], recv_sem=recv.at[r, bb],
            device_id={"blk": dst_b, "rep": dst_r}, device_id_type=MESH,
        )

    other = b + 1 - 2 * parity

    @pl.loop(0, quads)
    def _(i):
        bb = 2 * lax.rem(own_q + i, quads) + parity
        landed(r, bb).wait()
        forward(bb, ysend, other, r).start()
        forward(bb, fsend, b, sib).start()

    @pl.loop(0, quads)
    def _(i):
        bb = 2 * lax.rem(own_q + i, quads) + 1 - parity
        landed(r, bb).wait()
        forward(bb, fsend, b, sib).start()

    @pl.loop(0, blks)
    def _(bb):
        landed(sib, bb).wait()

    m = reps * blks * CAP
    gate_acc = jnp.zeros((m, wg.shape[1]), jnp.float32)
    up_acc = jnp.zeros((m, wg.shape[1]), jnp.float32)
    for k in range(kchunks):
        for copy in k_copies(k):
            copy.wait()
        at = slice(k * kc, (k + 1) * kc)
        x = rows[:, :, :, at].reshape(m, kc)
        gate_acc = gate_acc + jnp.dot(x, wg[at, :], preferred_element_type=jnp.float32)
        up_acc = up_acc + jnp.dot(x, wu[at, :], preferred_element_type=jnp.float32)
    hidden = (gate_acc / (1.0 + jnp.exp(-gate_acc)) * up_acc).astype(jnp.bfloat16)

    mh = m // reps

    def swap(n):
        at = pl.ds(n * nc, nc)
        return pltpu.make_async_remote_copy(
            src_ref=give.at[:, at], dst_ref=got.at[:, at],
            send_sem=xsend.at[n], recv_sem=xrecv.at[n],
            device_id={"blk": b, "rep": sib}, device_id_type=MESH,
        )

    def send_back(n, bb):
        at = pl.ds(n * nc, nc)
        return pltpu.make_async_remote_copy(
            src_ref=back.at[bb, :, at], dst_ref=returned.at[b, :, at],
            send_sem=bsend.at[n, bb], recv_sem=brecv.at[n, b],
            device_id={"blk": bb, "rep": r}, device_id_type=MESH,
        )

    def keep_back(n):
        at = pl.ds(n * nc, nc)
        return pltpu.make_async_copy(
            back.at[b, :, at], returned.at[b, :, at], brecv.at[n, b]
        )

    for n in range(nchunks):
        d_copy(n).wait()
        at = slice(n * nc, (n + 1) * nc)
        part = jnp.dot(hidden, wd[:, at], preferred_element_type=jnp.float32)
        low, high = part[:mh], part[mh:]
        keep[:, at] = jnp.where(r == 0, low, high)
        give[:, at] = jnp.where(r == 0, high, low).astype(jnp.bfloat16)
        swap(n).start()

    for n in range(nchunks):
        swap(n).wait_recv()
        at = slice(n * nc, (n + 1) * nc)
        total = (keep[:, at] + got[:, at].astype(jnp.float32)).astype(jnp.bfloat16)
        back[:, :, at] = total.reshape(blks, CAP, nc)
        keep_back(n).start()

        @pl.loop(1, blks)
        def _(i):
            send_back(n, lax.rem(b + i, blks)).start()

    weights = weight_buf[...]
    for n in range(nchunks):
        at = slice(n * nc, (n + 1) * nc)

        @pl.loop(0, blks)
        def _(bb):
            ref = returned.at[bb, :, pl.ds(n * nc, nc)]
            pltpu.make_async_copy(ref, ref, brecv.at[n, bb]).wait()

        acc = jnp.zeros((t_count, nc), jnp.float32)
        for e in range(experts):
            value = returned[e * group, :, at].astype(jnp.float32)
            for i in range(1, group):
                value = value + returned[e * group + i, :, at].astype(jnp.float32)
            for c in range(CAP):
                j = e * CAP + c
                acc = acc + weights[:, j : j + 1] * value[c : c + 1, :]
        out_ref[:, at] = acc.astype(jnp.bfloat16)

    @pl.loop(0, experts)
    def _(e):
        @pl.loop(0, half)
        def _(h):
            dst, copy = first(e, h)

            @pl.when(dst != b)
            def _():
                copy.wait_send()

    @pl.loop(0, quads)
    def _(i):
        forward(2 * i + parity, ysend, other, r).wait_send()

    @pl.loop(0, blks)
    def _(bb):
        forward(bb, fsend, b, sib).wait_send()

    for n in range(nchunks):
        swap(n).wait_send()

        @pl.loop(1, blks)
        def _(i):
            send_back(n, lax.rem(b + i, blks)).wait_send()


def shards(tokens, router_scores, expert_ids, gate_weight, up_weight, down_weight):
    blks = lax.axis_size("blk")
    reps = lax.axis_size("rep")
    t_count, width = tokens.shape
    units = gate_weight.shape[1]
    experts = blks * reps * units // FF
    kchunks, nchunks = 4, 4
    bf16, f32 = jnp.bfloat16, jnp.float32
    dma = pltpu.SemaphoreType.DMA
    vmem = pl.BlockSpec(memory_space=pltpu.VMEM)
    hbm = pl.BlockSpec(memory_space=pl.ANY)
    return pl.pallas_call(
        functools.partial(kernel, blks, reps, experts, kchunks, nchunks),
        out_shape=jax.ShapeDtypeStruct((t_count, width), bf16),
        in_specs=[vmem, vmem, hbm, hbm, hbm, hbm],
        out_specs=vmem,
        scratch_shapes=[
            pltpu.VMEM((t_count, width), bf16),
            pltpu.VMEM((width, units), bf16),
            pltpu.VMEM((width, units), bf16),
            pltpu.VMEM((units, width), bf16),
            pltpu.VMEM((experts, CAP, width), bf16),
            pltpu.VMEM((reps, blks, CAP, width), bf16),
            pltpu.VMEM((blks * CAP, width), f32),
            pltpu.VMEM((blks * CAP, width), bf16),
            pltpu.VMEM((blks * CAP, width), bf16),
            pltpu.VMEM((blks, CAP, width), bf16),
            pltpu.VMEM((blks, CAP, width), bf16),
            pltpu.VMEM((t_count, experts * CAP), f32),
            dma(()),
            dma((2, kchunks)),
            dma((nchunks,)),
            dma((blks // 2,)),
            dma((reps, blks)),
            dma((blks,)),
            dma((blks,)),
            dma((nchunks,)),
            dma((nchunks,)),
            dma((nchunks, blks)),
            dma((nchunks, blks)),
        ],
        compiler_params=pltpu.CompilerParams(
            collective_id=0, has_side_effects=True, vmem_limit_bytes=60000 * 1024
        ),
    )(router_scores, expert_ids, tokens, gate_weight, up_weight, down_weight)


def solution(mesh):
    placed = (
        P(("groups", "blk", "rep"), None),
        P(("groups", "blk", "rep"), None),
        P(("groups", "blk", "rep"), None),
        P(None, ("blk", "rep")),
        P(None, ("blk", "rep")),
        P(("blk", "rep"), None),
    )
    return jax.shard_map(
        shards,
        mesh=mesh,
        in_specs=placed,
        out_specs=P(("groups", "blk", "rep"), None),
        check_vma=False,
    )
```

```python
import functools

import jax
import jax.numpy as jnp
from jax import lax
from jax.experimental import pallas as pl
from jax.experimental.pallas import tpu as pltpu
from jax.sharding import PartitionSpec as P

FF = 2048
CAP = 2
MESH = pl.DeviceIdType.MESH

route_scale = 2.5


def kernel(
    blks, reps, experts, kchunks, nchunks,
    scores_hbm, ids_hbm, tok_hbm, gate_hbm, up_hbm, down_hbm, out_ref,
    scores_ref, ids_ref, tok, wg, wu, wd, packed, rows, keep, give, got, back, returned, weight_buf,
    route_sem, tok_sem, w_sem, d_sem, dsend, recv, fsend, ysend, xsend, xrecv, bsend, brecv,
):
    b = lax.axis_index("blk")
    r = lax.axis_index("rep")
    sib = 1 - r
    group = blks // experts
    half = group // 2
    width = tok.shape[1]
    slots = experts * CAP
    kc = width // kchunks
    nc = width // nchunks
    parity = lax.rem(b, 2)
    own_q = lax.div(b, 2)
    own_expert = lax.div(b, group)
    quads = blks // 2

    barrier = pltpu.get_barrier_semaphore()
    other = b + 1 - 2 * parity

    def greet(bb, rr):
        pl.semaphore_signal(
            barrier, inc=1, device_id={"blk": bb, "rep": rr}, device_id_type=MESH
        )

    @pl.loop(1, quads)
    def _(i):
        greet(2 * lax.rem(own_q + i, quads) + parity, r)

    greet(other, r)
    greet(b, sib)

    route_copies = (
        pltpu.make_async_copy(scores_hbm, scores_ref, route_sem.at[0]),
        pltpu.make_async_copy(ids_hbm, ids_ref, route_sem.at[1]),
    )
    for copy in route_copies:
        copy.start()
    tok_copy = pltpu.make_async_copy(tok_hbm, tok, tok_sem)
    tok_copy.start()

    def k_copies(k):
        at = pl.ds(k * kc, kc)
        return (
            pltpu.make_async_copy(gate_hbm.at[at, :], wg.at[at, :], w_sem.at[0, k]),
            pltpu.make_async_copy(up_hbm.at[at, :], wu.at[at, :], w_sem.at[1, k]),
        )

    def d_copy(n):
        at = pl.ds(n * nc, nc)
        return pltpu.make_async_copy(down_hbm.at[:, at], wd.at[:, at], d_sem.at[n])

    for k in range(kchunks):
        for copy in k_copies(k):
            copy.start()
    for n in range(nchunks):
        d_copy(n).start()

    for copy in route_copies:
        copy.wait()
    sig = jax.nn.sigmoid(scores_ref[...])
    gates = route_scale * sig / jnp.sum(sig, axis=0, keepdims=True)
    ids = ids_ref[...]
    t_count = ids.shape[1]
    slot = lax.broadcasted_iota(jnp.int32, (slots, t_count), 0)
    slot_expert = lax.div(slot, CAP)
    slot_rank = (slot - slot_expert * CAP).astype(jnp.float32)
    hit = jnp.zeros((slots, t_count), jnp.float32)
    weight = jnp.zeros((slots, t_count), jnp.float32)
    for j in range(ids.shape[0]):
        same = ids[j : j + 1, :] == slot_expert
        hit = hit + jnp.where(same, 1.0, 0.0)
        weight = weight + jnp.where(same, gates[j : j + 1, :], 0.0)
    row_i = lax.broadcasted_iota(jnp.int32, (t_count, t_count), 0)
    col_i = lax.broadcasted_iota(jnp.int32, (t_count, t_count), 1)
    upto = jnp.where(row_i <= col_i, 1.0, 0.0).astype(jnp.bfloat16)
    rank = jnp.dot(hit.astype(jnp.bfloat16), upto, preferred_element_type=jnp.float32) - 1.0
    placed = jnp.where(rank == slot_rank, hit, 0.0)
    tok_copy.wait()
    picked = jnp.dot(
        placed.astype(jnp.bfloat16), tok[...], preferred_element_type=jnp.float32
    ).astype(jnp.bfloat16)
    for e in range(experts):
        packed[e] = picked[e * CAP : (e + 1) * CAP, :]

    pl.semaphore_wait(barrier, quads + 1)

    def first(e, h):
        dst = e * group + 2 * h + parity
        copy = pltpu.make_async_remote_copy(
            src_ref=packed.at[e], dst_ref=rows.at[r, b],
            send_sem=dsend.at[e * half + h], recv_sem=recv.at[r, b],
            device_id={"blk": dst, "rep": r}, device_id_type=MESH,
        )
        return dst, copy

    own_copy = pltpu.make_async_copy(packed.at[own_expert], rows.at[r, b], recv.at[r, b])
    own_copy.start()

    @pl.loop(0, experts)
    def _(e):
        @pl.loop(0, half)
        def _(h):
            dst, copy = first(e, h)

            @pl.when(dst != b)
            def _():
                copy.start()

    slot_weight = placed * weight
    for j in range(slots):
        spread = jnp.where(row_i == col_i, slot_weight[j : j + 1, :], 0.0)
        weight_buf[:, j : j + 1] = jnp.sum(spread, axis=1, keepdims=True)

    def landed(rr, bb):
        return pltpu.make_async_copy(rows.at[rr, bb], rows.at[rr, bb], recv.at[rr, bb])

    def forward(bb, sems, dst_b, dst_r):
        return pltpu.make_async_remote_copy(
            src_ref=rows.at[r, bb], dst_ref=rows.at[r, bb],
            send_sem=sems.at[bb], recv_sem=recv.at[r, bb],
            device_id={"blk": dst_b, "rep": dst_r}, device_id_type=MESH,
        )

    @pl.loop(0, quads)
    def _(i):
        bb = 2 * lax.rem(own_q + i, quads) + parity
        landed(r, bb).wait()
        forward(bb, ysend, other, r).start()
        forward(bb, fsend, b, sib).start()

    @pl.loop(0, quads)
    def _(i):
        bb = 2 * lax.rem(own_q + i, quads) + 1 - parity
        landed(r, bb).wait()
        forward(bb, fsend, b, sib).start()

    @pl.loop(0, blks)
    def _(bb):
        landed(sib, bb).wait()

    m = reps * blks * CAP
    gate_acc = jnp.zeros((m, wg.shape[1]), jnp.float32)
    up_acc = jnp.zeros((m, wg.shape[1]), jnp.float32)
    for k in range(kchunks):
        for copy in k_copies(k):
            copy.wait()
        at = slice(k * kc, (k + 1) * kc)
        x = rows[:, :, :, at].reshape(m, kc)
        gate_acc = gate_acc + jnp.dot(x, wg[at, :], preferred_element_type=jnp.float32)
        up_acc = up_acc + jnp.dot(x, wu[at, :], preferred_element_type=jnp.float32)
    hidden = (gate_acc / (1.0 + jnp.exp(-gate_acc)) * up_acc).astype(jnp.bfloat16)

    mh = m // reps

    def swap(n):
        at = pl.ds(n * nc, nc)
        return pltpu.make_async_remote_copy(
            src_ref=give.at[:, at], dst_ref=got.at[:, at],
            send_sem=xsend.at[n], recv_sem=xrecv.at[n],
            device_id={"blk": b, "rep": sib}, device_id_type=MESH,
        )

    def send_back(n, bb):
        at = pl.ds(n * nc, nc)
        return pltpu.make_async_remote_copy(
            src_ref=back.at[bb, :, at], dst_ref=returned.at[b, :, at],
            send_sem=bsend.at[n, bb], recv_sem=brecv.at[n, b],
            device_id={"blk": bb, "rep": r}, device_id_type=MESH,
        )

    def keep_back(n):
        at = pl.ds(n * nc, nc)
        return pltpu.make_async_copy(
            back.at[b, :, at], returned.at[b, :, at], brecv.at[n, b]
        )

    for n in range(nchunks):
        d_copy(n).wait()
        at = slice(n * nc, (n + 1) * nc)
        part = jnp.dot(hidden, wd[:, at], preferred_element_type=jnp.float32)
        low, high = part[:mh], part[mh:]
        keep[:, at] = jnp.where(r == 0, low, high)
        give[:, at] = jnp.where(r == 0, high, low).astype(jnp.bfloat16)
        swap(n).start()

    for n in range(nchunks):
        swap(n).wait_recv()
        at = slice(n * nc, (n + 1) * nc)
        total = (keep[:, at] + got[:, at].astype(jnp.float32)).astype(jnp.bfloat16)
        back[:, :, at] = total.reshape(blks, CAP, nc)
        keep_back(n).start()

        @pl.loop(1, blks)
        def _(i):
            send_back(n, lax.rem(b + i, blks)).start()

    weights = weight_buf[...]
    for n in range(nchunks):
        at = slice(n * nc, (n + 1) * nc)

        @pl.loop(0, blks)
        def _(bb):
            ref = returned.at[bb, :, pl.ds(n * nc, nc)]
            pltpu.make_async_copy(ref, ref, brecv.at[n, bb]).wait()

        acc = jnp.zeros((t_count, nc), jnp.float32)
        for e in range(experts):
            value = returned[e * group, :, at].astype(jnp.float32)
            for i in range(1, group):
                value = value + returned[e * group + i, :, at].astype(jnp.float32)
            for c in range(CAP):
                j = e * CAP + c
                acc = acc + weights[:, j : j + 1] * value[c : c + 1, :]
        out_ref[:, at] = acc.astype(jnp.bfloat16)

    @pl.loop(0, experts)
    def _(e):
        @pl.loop(0, half)
        def _(h):
            dst, copy = first(e, h)

            @pl.when(dst != b)
            def _():
                copy.wait_send()

    @pl.loop(0, quads)
    def _(i):
        forward(2 * i + parity, ysend, other, r).wait_send()

    @pl.loop(0, blks)
    def _(bb):
        forward(bb, fsend, b, sib).wait_send()

    for n in range(nchunks):
        swap(n).wait_send()

        @pl.loop(1, blks)
        def _(i):
            send_back(n, lax.rem(b + i, blks)).wait_send()


def shards(tokens, router_scores, expert_ids, gate_weight, up_weight, down_weight):
    blks = lax.axis_size("blk")
    reps = lax.axis_size("rep")
    t_count, width = tokens.shape
    units = gate_weight.shape[1]
    experts = blks * reps * units // FF
    kchunks, nchunks = 4, 4
    bf16, f32 = jnp.bfloat16, jnp.float32
    dma = pltpu.SemaphoreType.DMA
    vmem = pl.BlockSpec(memory_space=pltpu.VMEM)
    hbm = pl.BlockSpec(memory_space=pl.ANY)
    in_hbm = lambda array: pltpu.with_memory_space_constraint(array, pltpu.HBM)
    row_bytes = 2 * width
    limit = (
        3 * units * row_bytes
        + (2 * t_count + 12 * blks * CAP + experts * CAP) * row_bytes
        + (8 << 20)
    )
    return pl.pallas_call(
        functools.partial(kernel, blks, reps, experts, kchunks, nchunks),
        out_shape=jax.ShapeDtypeStruct((t_count, width), bf16),
        in_specs=[hbm] * 6,
        out_specs=vmem,
        scratch_shapes=[
            pltpu.VMEM(router_scores.shape[::-1], f32),
            pltpu.VMEM(expert_ids.shape[::-1], jnp.int32),
            pltpu.VMEM((t_count, width), bf16),
            pltpu.VMEM((width, units), bf16),
            pltpu.VMEM((width, units), bf16),
            pltpu.VMEM((units, width), bf16),
            pltpu.VMEM((experts, CAP, width), bf16),
            pltpu.VMEM((reps, blks, CAP, width), bf16),
            pltpu.VMEM((blks * CAP, width), f32),
            pltpu.VMEM((blks * CAP, width), bf16),
            pltpu.VMEM((blks * CAP, width), bf16),
            pltpu.VMEM((blks, CAP, width), bf16),
            pltpu.VMEM((blks, CAP, width), bf16),
            pltpu.VMEM((t_count, experts * CAP), f32),
            dma((2,)),
            dma(()),
            dma((2, kchunks)),
            dma((nchunks,)),
            dma((blks // 2,)),
            dma((reps, blks)),
            dma((blks,)),
            dma((blks,)),
            dma((nchunks,)),
            dma((nchunks,)),
            dma((nchunks, blks)),
            dma((nchunks, blks)),
        ],
        compiler_params=pltpu.CompilerParams(
            collective_id=0, has_side_effects=True, vmem_limit_bytes=limit
        ),
    )(
        *map(
            in_hbm,
            (router_scores.T, expert_ids.T, tokens, gate_weight, up_weight, down_weight),
        )
    )


def solution(mesh):
    placed = (
        P(("groups", "blk", "rep"), None),
        P(("groups", "blk", "rep"), None),
        P(("groups", "blk", "rep"), None),
        P(None, ("blk", "rep")),
        P(None, ("blk", "rep")),
        P(("blk", "rep"), None),
    )
    return jax.shard_map(
        shards,
        mesh=mesh,
        in_specs=placed,
        out_specs=P(("groups", "blk", "rep"), None),
        check_vma=False,
    )
```

```python
import functools

import jax
import jax.numpy as jnp
from jax import lax
from jax.experimental import pallas as pl
from jax.experimental.pallas import tpu as pltpu
from jax.sharding import PartitionSpec as P

FF = 2048
CAP = 2
MESH = pl.DeviceIdType.MESH

route_scale = 2.5


def kernel(
    blks, reps, experts, kchunks, nchunks,
    scores_hbm, ids_hbm, tok_hbm, gate_hbm, up_hbm, down_hbm, out_ref,
    scores_ref, ids_ref, tok, wg, wu, wd, packed, rows, keep, give, got, back, returned, weight_buf,
    route_sem, tok_sem, w_sem, d_sem, dsend, recv, fsend, ysend, xsend, xrecv, bsend, brecv,
):
    b = lax.axis_index("blk")
    r = lax.axis_index("rep")
    sib = 1 - r
    group = blks // experts
    half = group // 2
    width = tok.shape[1]
    slots = experts * CAP
    kc = width // kchunks
    nc = width // nchunks
    parity = lax.rem(b, 2)
    own_q = lax.div(b, 2)
    own_expert = lax.div(b, group)
    quads = blks // 2

    barrier = pltpu.get_barrier_semaphore()
    other = b + 1 - 2 * parity

    def greet(bb, rr):
        pl.semaphore_signal(
            barrier, inc=1, device_id={"blk": bb, "rep": rr}, device_id_type=MESH
        )

    @pl.loop(1, quads)
    def _(i):
        greet(2 * lax.rem(own_q + i, quads) + parity, r)

    greet(other, r)
    greet(b, sib)

    route_copies = (
        pltpu.make_async_copy(scores_hbm, scores_ref, route_sem.at[0]),
        pltpu.make_async_copy(ids_hbm, ids_ref, route_sem.at[1]),
    )
    for copy in route_copies:
        copy.start()
    tok_copy = pltpu.make_async_copy(tok_hbm, tok, tok_sem)
    tok_copy.start()

    def k_copies(k):
        at = pl.ds(k * kc, kc)
        return (
            pltpu.make_async_copy(gate_hbm.at[at, :], wg.at[at, :], w_sem.at[0, k]),
            pltpu.make_async_copy(up_hbm.at[at, :], wu.at[at, :], w_sem.at[1, k]),
        )

    def d_copy(n):
        at = pl.ds(n * nc, nc)
        return pltpu.make_async_copy(down_hbm.at[:, at], wd.at[:, at], d_sem.at[n])


    for copy in route_copies:
        copy.wait()
    sig = jax.nn.sigmoid(scores_ref[...])
    gates = route_scale * sig / jnp.sum(sig, axis=0, keepdims=True)
    ids = ids_ref[...]
    t_count = ids.shape[1]
    slot = lax.broadcasted_iota(jnp.int32, (slots, t_count), 0)
    slot_expert = lax.div(slot, CAP)
    slot_rank = (slot - slot_expert * CAP).astype(jnp.float32)
    hit = jnp.zeros((slots, t_count), jnp.float32)
    weight = jnp.zeros((slots, t_count), jnp.float32)
    for j in range(ids.shape[0]):
        same = ids[j : j + 1, :] == slot_expert
        hit = hit + jnp.where(same, 1.0, 0.0)
        weight = weight + jnp.where(same, gates[j : j + 1, :], 0.0)
    row_i = lax.broadcasted_iota(jnp.int32, (t_count, t_count), 0)
    col_i = lax.broadcasted_iota(jnp.int32, (t_count, t_count), 1)
    upto = jnp.where(row_i <= col_i, 1.0, 0.0).astype(jnp.bfloat16)
    rank = jnp.dot(hit.astype(jnp.bfloat16), upto, preferred_element_type=jnp.float32) - 1.0
    placed = jnp.where(rank == slot_rank, hit, 0.0)
    tok_copy.wait()
    picked = jnp.dot(
        placed.astype(jnp.bfloat16), tok[...], preferred_element_type=jnp.float32
    ).astype(jnp.bfloat16)
    for e in range(experts):
        packed[e] = picked[e * CAP : (e + 1) * CAP, :]

    pl.semaphore_wait(barrier, quads + 1)

    def first(e, h):
        dst = e * group + 2 * h + parity
        copy = pltpu.make_async_remote_copy(
            src_ref=packed.at[e], dst_ref=rows.at[r, b],
            send_sem=dsend.at[e * half + h], recv_sem=recv.at[r, b],
            device_id={"blk": dst, "rep": r}, device_id_type=MESH,
        )
        return dst, copy

    own_copy = pltpu.make_async_copy(packed.at[own_expert], rows.at[r, b], recv.at[r, b])
    own_copy.start()

    @pl.loop(0, experts)
    def _(e):
        @pl.loop(0, half)
        def _(h):
            dst, copy = first(e, h)

            @pl.when(dst != b)
            def _():
                copy.start()

    for k in range(kchunks):
        for copy in k_copies(k):
            copy.start()
    for n in range(nchunks):
        d_copy(n).start()
    slot_weight = placed * weight
    for j in range(slots):
        spread = jnp.where(row_i == col_i, slot_weight[j : j + 1, :], 0.0)
        weight_buf[:, j : j + 1] = jnp.sum(spread, axis=1, keepdims=True)

    def landed(rr, bb):
        return pltpu.make_async_copy(rows.at[rr, bb], rows.at[rr, bb], recv.at[rr, bb])

    def forward(bb, sems, dst_b, dst_r):
        return pltpu.make_async_remote_copy(
            src_ref=rows.at[r, bb], dst_ref=rows.at[r, bb],
            send_sem=sems.at[bb], recv_sem=recv.at[r, bb],
            device_id={"blk": dst_b, "rep": dst_r}, device_id_type=MESH,
        )

    @pl.loop(0, quads)
    def _(i):
        bb = 2 * lax.rem(own_q + i, quads) + parity
        landed(r, bb).wait()
        forward(bb, ysend, other, r).start()
        forward(bb, fsend, b, sib).start()

    @pl.loop(0, quads)
    def _(i):
        bb = 2 * lax.rem(own_q + i, quads) + 1 - parity
        landed(r, bb).wait()
        forward(bb, fsend, b, sib).start()

    @pl.loop(0, blks)
    def _(bb):
        landed(sib, bb).wait()

    m = reps * blks * CAP
    gate_acc = jnp.zeros((m, wg.shape[1]), jnp.float32)
    up_acc = jnp.zeros((m, wg.shape[1]), jnp.float32)
    for k in range(kchunks):
        for copy in k_copies(k):
            copy.wait()
        at = slice(k * kc, (k + 1) * kc)
        x = rows[:, :, :, at].reshape(m, kc)
        gate_acc = gate_acc + jnp.dot(x, wg[at, :], preferred_element_type=jnp.float32)
        up_acc = up_acc + jnp.dot(x, wu[at, :], preferred_element_type=jnp.float32)
    hidden = (gate_acc / (1.0 + jnp.exp(-gate_acc)) * up_acc).astype(jnp.bfloat16)

    mh = m // reps

    def swap(n):
        at = pl.ds(n * nc, nc)
        return pltpu.make_async_remote_copy(
            src_ref=give.at[:, at], dst_ref=got.at[:, at],
            send_sem=xsend.at[n], recv_sem=xrecv.at[n],
            device_id={"blk": b, "rep": sib}, device_id_type=MESH,
        )

    def send_back(n, bb):
        at = pl.ds(n * nc, nc)
        return pltpu.make_async_remote_copy(
            src_ref=back.at[bb, :, at], dst_ref=returned.at[b, :, at],
            send_sem=bsend.at[n, bb], recv_sem=brecv.at[n, b],
            device_id={"blk": bb, "rep": r}, device_id_type=MESH,
        )

    def keep_back(n):
        at = pl.ds(n * nc, nc)
        return pltpu.make_async_copy(
            back.at[b, :, at], returned.at[b, :, at], brecv.at[n, b]
        )

    for n in range(nchunks):
        d_copy(n).wait()
        at = slice(n * nc, (n + 1) * nc)
        part = jnp.dot(hidden, wd[:, at], preferred_element_type=jnp.float32)
        low, high = part[:mh], part[mh:]
        keep[:, at] = jnp.where(r == 0, low, high)
        give[:, at] = jnp.where(r == 0, high, low).astype(jnp.bfloat16)
        swap(n).start()

    for n in range(nchunks):
        swap(n).wait_recv()
        at = slice(n * nc, (n + 1) * nc)
        total = (keep[:, at] + got[:, at].astype(jnp.float32)).astype(jnp.bfloat16)
        back[:, :, at] = total.reshape(blks, CAP, nc)
        keep_back(n).start()

        @pl.loop(1, blks)
        def _(i):
            send_back(n, lax.rem(b + i, blks)).start()

    weights = weight_buf[...]
    for n in range(nchunks):
        at = slice(n * nc, (n + 1) * nc)

        @pl.loop(0, blks)
        def _(bb):
            ref = returned.at[bb, :, pl.ds(n * nc, nc)]
            pltpu.make_async_copy(ref, ref, brecv.at[n, bb]).wait()

        acc = jnp.zeros((t_count, nc), jnp.float32)
        for e in range(experts):
            value = returned[e * group, :, at].astype(jnp.float32)
            for i in range(1, group):
                value = value + returned[e * group + i, :, at].astype(jnp.float32)
            for c in range(CAP):
                j = e * CAP + c
                acc = acc + weights[:, j : j + 1] * value[c : c + 1, :]
        out_ref[:, at] = acc.astype(jnp.bfloat16)

    @pl.loop(0, experts)
    def _(e):
        @pl.loop(0, half)
        def _(h):
            dst, copy = first(e, h)

            @pl.when(dst != b)
            def _():
                copy.wait_send()

    @pl.loop(0, quads)
    def _(i):
        forward(2 * i + parity, ysend, other, r).wait_send()

    @pl.loop(0, blks)
    def _(bb):
        forward(bb, fsend, b, sib).wait_send()

    for n in range(nchunks):
        swap(n).wait_send()

        @pl.loop(1, blks)
        def _(i):
            send_back(n, lax.rem(b + i, blks)).wait_send()


def shards(tokens, router_scores, expert_ids, gate_weight, up_weight, down_weight):
    blks = lax.axis_size("blk")
    reps = lax.axis_size("rep")
    t_count, width = tokens.shape
    units = gate_weight.shape[1]
    experts = blks * reps * units // FF
    kchunks, nchunks = 4, 2
    bf16, f32 = jnp.bfloat16, jnp.float32
    dma = pltpu.SemaphoreType.DMA
    vmem = pl.BlockSpec(memory_space=pltpu.VMEM)
    hbm = pl.BlockSpec(memory_space=pl.ANY)
    in_hbm = lambda array: pltpu.with_memory_space_constraint(array, pltpu.HBM)
    row_bytes = 2 * width
    limit = (
        3 * units * row_bytes
        + (2 * t_count + 12 * blks * CAP + experts * CAP) * row_bytes
        + (8 << 20)
    )
    return pl.pallas_call(
        functools.partial(kernel, blks, reps, experts, kchunks, nchunks),
        out_shape=jax.ShapeDtypeStruct((t_count, width), bf16),
        in_specs=[hbm] * 6,
        out_specs=vmem,
        scratch_shapes=[
            pltpu.VMEM(router_scores.shape[::-1], f32),
            pltpu.VMEM(expert_ids.shape[::-1], jnp.int32),
            pltpu.VMEM((t_count, width), bf16),
            pltpu.VMEM((width, units), bf16),
            pltpu.VMEM((width, units), bf16),
            pltpu.VMEM((units, width), bf16),
            pltpu.VMEM((experts, CAP, width), bf16),
            pltpu.VMEM((reps, blks, CAP, width), bf16),
            pltpu.VMEM((blks * CAP, width), f32),
            pltpu.VMEM((blks * CAP, width), bf16),
            pltpu.VMEM((blks * CAP, width), bf16),
            pltpu.VMEM((blks, CAP, width), bf16),
            pltpu.VMEM((blks, CAP, width), bf16),
            pltpu.VMEM((t_count, experts * CAP), f32),
            dma((2,)),
            dma(()),
            dma((2, kchunks)),
            dma((nchunks,)),
            dma((blks // 2,)),
            dma((reps, blks)),
            dma((blks,)),
            dma((blks,)),
            dma((nchunks,)),
            dma((nchunks,)),
            dma((nchunks, blks)),
            dma((nchunks, blks)),
        ],
        compiler_params=pltpu.CompilerParams(
            collective_id=0, has_side_effects=True, vmem_limit_bytes=limit
        ),
    )(
        *map(
            in_hbm,
            (router_scores.T, expert_ids.T, tokens, gate_weight, up_weight, down_weight),
        )
    )


def solution(mesh):
    placed = (
        P(("groups", "blk", "rep"), None),
        P(("groups", "blk", "rep"), None),
        P(("groups", "blk", "rep"), None),
        P(None, ("blk", "rep")),
        P(None, ("blk", "rep")),
        P(("blk", "rep"), None),
    )
    return jax.shard_map(
        shards,
        mesh=mesh,
        in_specs=placed,
        out_specs=P(("groups", "blk", "rep"), None),
        check_vma=False,
    )
```
